128 devices in a mesh: ex: 16 (over x, z), tp: 4 (over y), dp: 2 (over core).
Axes of the slice: x: 4, y: 4, z: 4, core: 2. Of those that a mesh axis runs over, the one named last changes fastest.
Arguments:
- tokens: bfloat16 [4096, 2880], P(('ex', 'dp')), may hold values from -32 to 32
- route_one: int32 [4096, 4], P(('ex', 'dp')), may hold values from 0 to 15, as said below
- route_two: int32 [4096, 4], P(('ex', 'dp')), may hold values from 0 to 15, as said below
- share_one: float32 [4096, 4], P(('ex', 'dp')), may hold values from 0.05 to 0.6
- share_two: float32 [4096, 4], P(('ex', 'dp')), may hold values from 0.05 to 0.6
- gain_one: float32 [2880], replicated, may hold values from 0.5 to 1.5
- gain_two: float32 [2880], replicated, may hold values from 0.5 to 1.5
- gate_up_one: bfloat16 [16, 2880, 2, 2880], P('ex', None, None, 'tp'), may hold values from -0.109375 to 0.109375
- down_one: bfloat16 [16, 2880, 2880], P('ex', 'tp'), may hold values from -0.109375 to 0.109375
- gate_up_two: bfloat16 [16, 2880, 2, 2880], P('ex', None, None, 'tp'), may hold values from -0.109375 to 0.109375
- down_two: bfloat16 [16, 2880, 2880], P('ex', 'tp'), may hold values from -0.109375 to 0.109375
Outputs:
- mixed: bfloat16 [4096, 2880], P(('ex', 'dp'), 'tp')
- load: int32 [2, 16], P(None, 'ex')
The draws below stay inside these ranges and needn't reach their ends.
Inputs may be any that keep to these rules, and one draw needn't show every extreme that they name: `route_one`: each row names 4 different experts; in each aligned block of 128 rows no expert is named by more than 64 rows, and in every block some expert is named by exactly 64 rows. `route_two`: each row names 4 different experts; in each aligned block of 128 rows no expert is named by more than 64 rows, and in every block some expert is named by exactly 64 rows.
All inputs are finite; a program needn't handle non-finite values.
Results may differ from the reference program's by a relative error of at most 0.011.
Values may be sent and summed in bfloat16 or wider, within the bound.
A program may use at most 128 MiB of HBM per device.

```python
import math
import jax
import jax.numpy as jnp
from jax import lax

D = 2880
FF = 2880
TOP = 4
EXPERTS = 16
TOK_DEV = 128
CAP = 64
TOKENS = 4096
N_TP = 4


def draw_tokens(key, part):
    key_rows, key_cols, key_base = jax.random.split(key, 3)
    row_scale = jnp.exp(jax.random.uniform(key_rows, (TOKENS, 1), jnp.float32, math.log(0.5), math.log(2.0)))
    col_scale = jnp.exp(jax.random.uniform(key_cols, (1, D), jnp.float32, math.log(0.4), math.log(4.0)))
    base = jax.random.truncated_normal(key_base, -4.0, 4.0, (TOKENS, D), jnp.float32)
    return (base * row_scale * col_scale).astype(jnp.bfloat16)


def route_table(key):
    blocks = TOKENS // TOK_DEV
    quarter = CAP // 4
    global_order = jax.random.permutation(jax.random.fold_in(key, 7), EXPERTS)
    position = jnp.zeros((EXPERTS,), jnp.int32).at[global_order].set(jnp.arange(EXPERTS, dtype=jnp.int32))
    first_half = position < EXPERTS // 2

    def one_block(block):
        block_key = jax.random.fold_in(key, block + 11)
        key_order, key_rows = jax.random.split(block_key)
        odd = block % 2 == 1
        heavy = jnp.logical_xor(first_half, odd)
        counts = jnp.where(heavy, 3 * quarter, quarter).astype(jnp.int32)
        order = jax.random.permutation(key_order, EXPERTS).astype(jnp.int32)
        heavy_ordered = heavy[order].astype(jnp.int32)
        seen = jnp.cumsum(heavy_ordered)
        adjust = jnp.where((heavy_ordered == 1) & (seen == 1), quarter, 0) - jnp.where((heavy_ordered == 1) & (seen == 2), quarter, 0)
        ordered_counts = counts[order] + adjust.astype(jnp.int32)
        listed = jnp.repeat(order, ordered_counts, total_repeat_length=TOK_DEV * TOP)
        table = listed.reshape(TOP, TOK_DEV).T
        shuffle = jax.random.permutation(key_rows, TOK_DEV)
        return table[shuffle]
    tables = jax.vmap(one_block)(jnp.arange(blocks, dtype=jnp.int32))
    return tables.reshape(TOKENS, TOP).astype(jnp.int32)


def draw_route_one(key, part):
    return route_table(jax.random.fold_in(key, 101))


def draw_route_two(key, part):
    return route_table(jax.random.fold_in(key, 202))


def shard_levels(own_key, extent, cuts, smallest, largest):
    gain, own = 1.0, jax.random.fold_in(own_key, 6)
    for axis_at, shards_of in cuts:
        steps = jnp.exp(jax.random.uniform(jax.random.fold_in(own, axis_at), (shards_of,), jnp.float32, smallest / len(cuts), largest / len(cuts)))
        gain = gain * jnp.repeat(steps, extent[axis_at] // shards_of).reshape([-1 if axis == axis_at else 1 for axis in range(len(extent))])
    return gain


def centred(rng, shape, scale, most, cuts=(), held_as=jnp.bfloat16):
    loudness = shard_levels(rng, shape, cuts, -0.22, 0.18) if cuts else 1.0
    array = jax.random.normal(rng, shape, jnp.float32) * scale * loudness
    return jnp.minimum(jnp.maximum(array, -most), most).astype(held_as)


def setup_inputs(seed: int = 0) -> dict:
    seeds = jax.random.split(jax.random.key(seed), 12)
    return {
        "tokens": draw_tokens(jax.random.fold_in(seeds[11], 71), 0),
        "route_one": draw_route_one(jax.random.fold_in(seeds[11], 71), 0),
        "route_two": draw_route_two(jax.random.fold_in(seeds[11], 71), 0),
        "share_one": jnp.clip(0.05 + 0.55 * jax.random.uniform(seeds[3], (TOKENS, TOP), jnp.float32) ** shard_levels(seeds[3], (TOKENS, TOP), ((0, 32),), -0.2, 0.2), 0.05, 0.6),
        "share_two": jnp.clip(0.05 + 0.55 * jax.random.uniform(seeds[4], (TOKENS, TOP), jnp.float32) ** shard_levels(seeds[4], (TOKENS, TOP), ((0, 32),), -0.2, 0.2), 0.05, 0.6),
        "gain_one": jnp.clip(1.0 + 0.1 * jax.random.normal(seeds[5], (D,), jnp.float32), 0.5, 1.5),
        "gain_two": jnp.clip(1.0 + 0.1 * jax.random.normal(seeds[6], (D,), jnp.float32), 0.5, 1.5),
        "gate_up_one": centred(seeds[7], (EXPERTS, D, 2, FF), D ** -0.5, 0.109375, ((0, 16), (3, 4))),
        "down_one": centred(seeds[8], (EXPERTS, FF, D), FF ** -0.5, 0.109375, ((0, 16), (1, 4))),
        "gate_up_two": centred(seeds[9], (EXPERTS, D, 2, FF), D ** -0.5, 0.109375, ((0, 16), (3, 4))),
        "down_two": centred(seeds[10], (EXPERTS, FF, D), FF ** -0.5, 0.109375, ((0, 16), (1, 4))),
    }


norm_eps = 1e-05
glu_alpha = 1.702

def expert_layer(stream, routes, shares, gains, gate_up, down_proj):
    tokens_all = stream.shape[0]
    model_width = stream.shape[1]
    experts = gate_up.shape[0]
    hidden_width = gate_up.shape[3]
    top_count = routes.shape[1]
    blocks = tokens_all // TOK_DEV
    share_width = hidden_width // N_TP
    values = stream.astype(jnp.float32)
    inverse = lax.rsqrt(lax.optimization_barrier(jnp.mean(values * values, axis=1, keepdims=True)) + norm_eps)
    normed = (values * inverse * gains[None, :]).astype(jnp.bfloat16)
    flattened = routes.reshape(blocks, TOK_DEV * top_count)
    matches = (flattened[:, :, None] == jnp.arange(experts, dtype=jnp.int32)[None, None, :]).astype(jnp.int32)
    slot_rank = jnp.cumsum(matches, axis=1) - 1
    slot_index = lax.optimization_barrier(jnp.sum(slot_rank * matches, axis=2))
    target = (flattened * CAP + slot_index).astype(jnp.int32)
    block_index = jnp.broadcast_to(jnp.arange(blocks, dtype=jnp.int32)[:, None], target.shape)
    repeated = jnp.repeat(normed.reshape(blocks, TOK_DEV, model_width), top_count, axis=1)
    packed = jnp.zeros((blocks, experts * CAP, model_width), jnp.bfloat16).at[block_index, target].set(repeated)
    per_expert = packed.reshape(blocks, experts, CAP, model_width).transpose(1, 0, 2, 3).reshape(experts, blocks * CAP, model_width)

    def one_expert(operands):
        inputs, weight_in, weight_down = operands
        hidden = jnp.dot(inputs.astype(jnp.float32), weight_in.reshape(model_width, 2 * hidden_width).astype(jnp.float32), precision=lax.Precision.HIGHEST)
        gate_part = hidden[:, :hidden_width]
        up_part = hidden[:, hidden_width:]
        activated = (gate_part * jax.nn.sigmoid(glu_alpha * gate_part) * (up_part + 1.0)).astype(jnp.bfloat16)
        summed = jnp.zeros((inputs.shape[0], model_width), jnp.float32)
        for section in range(N_TP):
            lower = section * share_width
            upper = lower + share_width
            portion = jnp.dot(activated[:, lower:upper].astype(jnp.float32), weight_down[lower:upper].astype(jnp.float32), precision=lax.Precision.HIGHEST)
            rounded = lax.optimization_barrier(portion.astype(jnp.bfloat16))
            summed = summed + rounded.astype(jnp.float32)
        return summed.astype(jnp.bfloat16)
    outputs = lax.map(one_expert, (per_expert, gate_up, down_proj))
    returned = outputs.reshape(experts, blocks, CAP, model_width).transpose(1, 0, 2, 3).reshape(blocks, experts * CAP, model_width)
    picked = returned[block_index, target].astype(jnp.float32).reshape(tokens_all, top_count, model_width)
    mixed = values + lax.optimization_barrier(jnp.sum(shares[:, :, None] * picked, axis=1))
    counted = lax.optimization_barrier(jnp.sum(matches, axis=(0, 1))).astype(jnp.int32)
    return (mixed.astype(jnp.bfloat16), counted)

def reference(tokens, route_one, route_two, share_one, share_two, gain_one, gain_two, gate_up_one, down_one, gate_up_two, down_two):
    stream, load_first = expert_layer(tokens, route_one, share_one, gain_one, gate_up_one, down_one)
    mixed, load_second = expert_layer(stream, route_two, share_two, gain_two, gate_up_two, down_two)
    return (mixed, jnp.stack([load_first, load_second]))
```

```python
import functools

import jax
import jax.numpy as jnp
from jax import lax
from jax.experimental import pallas as pl
from jax.experimental.pallas import tpu as pltpu
from jax.sharding import PartitionSpec as P

MESH = pl.DeviceIdType.MESH
norm_eps = 1e-05
glu_alpha = 1.702
SIDE = 4
GROUPS = 4
NT = (((1,), (1,)), ((), ()))
TN = (((0,), (0,)), ((), ()))


def layer_kernel(last, cap, *refs):
    if last:
        (x_ref, rt_ref, st_ref, gain_ref, wgu_hbm, wd_hbm, out_ref, *scratch) = refs
    else:
        (x_ref, rt_ref, rt2_ref, st_ref, gain_ref, wgu_hbm, wd_hbm, out_ref, load_ref, *scratch) = refs
    (
        wgu, wd, normed, slots, shares, pk, arr, part, yr, half_buf, ret, acc, rs_send, rs_recv, w_sem,
        in_s, in_r, fw_s, fw_r, ex_s, ex_r, rt_s, rt_r, rs_s, rs_r, *more,
    ) = scratch
    tokens, width = x_ref.shape
    share_width = wd.shape[0]
    half_cap = cap // 2
    quarter = cap // 4
    rows = GROUPS * cap
    half_rows = GROUPS * half_cap

    me = lax.axis_index("ex")
    y = lax.axis_index("tp")
    c = lax.axis_index("dp")
    my_x, my_z = me // SIDE, me % SIDE
    odd = y % 2
    near = (y + 1 - 2 * odd + SIDE) % SIDE
    far = (y - 1 + 2 * odd + SIDE) % SIDE

    def expert_at(g, j):
        return ((my_x + j) % SIDE) * SIDE + (my_z + j + g) % SIDE

    def source_at(g, j):
        return ((my_x - j + SIDE) % SIDE) * SIDE + (my_z - j - g + 2 * SIDE) % SIDE

    def send(src, dst, s_sem, r_sem, device):
        return pltpu.make_async_remote_copy(
            src_ref=src, dst_ref=dst, send_sem=s_sem, recv_sem=r_sem, device_id=device, device_id_type=MESH
        )

    def al(v, m):
        return pl.multiple_of(v, m)

    barrier = pltpu.get_barrier_semaphore()
    for o in range(1, SIDE * GROUPS):
        pl.semaphore_signal(barrier, inc=1, device_id=(expert_at(o // 4, o % 4), y, c), device_id_type=MESH)
    for k in range(1, SIDE):
        pl.semaphore_signal(barrier, inc=1, device_id=(me, (y + k) % SIDE, c), device_id_type=MESH)
    if not last:
        pl.semaphore_signal(barrier, inc=1, device_id=(me, y, 1 - c), device_id_type=MESH)

    load_wgu = pltpu.make_async_copy(wgu_hbm, wgu, w_sem.at[0])
    load_wd = pltpu.make_async_copy(wd_hbm, wd, w_sem.at[1])
    load_wgu.start()
    load_wd.start()

    experts = slots.shape[0]
    expert_id = lax.broadcasted_iota(jnp.int32, (experts, tokens), 0)

    def chosen(table):
        hit = jnp.zeros((experts, tokens), jnp.float32)
        for k in range(table.shape[0]):
            hit = hit + jnp.where(table[k : k + 1, :] == expert_id, 1.0, 0.0)
        return hit

    table = rt_ref[...]
    hit = chosen(table)
    before = (
        lax.broadcasted_iota(jnp.int32, (tokens, tokens), 0) < lax.broadcasted_iota(jnp.int32, (tokens, tokens), 1)
    )
    rank = jnp.dot(
        hit.astype(jnp.bfloat16), jnp.where(before, 1.0, 0.0).astype(jnp.bfloat16), preferred_element_type=jnp.float32
    )
    slots[...] = jnp.where(hit > 0.5, rank, -1.0)
    weight = jnp.zeros((experts, tokens), jnp.float32)
    for k in range(table.shape[0]):
        weight = weight + jnp.where(table[k : k + 1, :] == expert_id, st_ref[k : k + 1, :], 0.0)
    shares[...] = weight

    gains = gain_ref[...]
    for r in range(0, tokens, 16):
        v = x_ref[r : r + 16, :].astype(jnp.float32)
        inverse = lax.rsqrt(jnp.mean(v * v, axis=1, keepdims=True) + norm_eps)
        normed[r : r + 16, :] = (v * inverse * gains).astype(jnp.bfloat16)

    if not last:
        hits, cnt_s_buf, cnt_r_buf, pair_s_buf, pair_r_buf, gathered, cs, cr, ag_s, ag_r = more
        hits[0] = hit
        hits[1] = chosen(rt2_ref[...])

    pl.semaphore_wait(barrier, (SIDE * GROUPS - 1) + (SIDE - 1) + (0 if last else 1))

    def in_copy(g, j, device):
        o = g * 4 + j
        at = pl.ds(al(o * cap + odd * half_cap, half_cap), half_cap)
        return send(pk.at[at], arr.at[at], in_s.at[o], in_r.at[o], device)

    slot_id = lax.broadcasted_iota(jnp.int32, (cap, tokens), 0).astype(jnp.float32)

    def pack(g, _):
        chooser = jnp.concatenate(
            [jnp.where(slots[pl.ds(expert_at(g, j), 1), :] == slot_id, 1.0, 0.0) for j in range(4)], axis=0
        ).astype(jnp.bfloat16)
        packed = jnp.dot(chooser, normed[...], preferred_element_type=jnp.float32).astype(jnp.bfloat16)
        pk[pl.ds(al(g * rows, rows), rows), :] = packed

        @pl.when(g == 0)
        def _():
            arr[0:cap, :] = packed[0:cap]

        for j in range(4):

            @pl.when(g * 4 + j > 0)
            def _():
                in_copy(g, j, (expert_at(g, j), y, c)).start()

        return 0

    lax.fori_loop(0, GROUPS, pack, 0)

    if not last:

        def count_copy(o, device):
            return send(cnt_s_buf.at[o], cnt_r_buf.at[o], cs.at[o], cr.at[o], device)

        row_id = lax.broadcasted_iota(jnp.int32, (8, 128), 0)

        def count_tile(e):
            one = jnp.sum(hits[0, pl.ds(e, 1), :], axis=1, keepdims=True)
            two = jnp.sum(hits[1, pl.ds(e, 1), :], axis=1, keepdims=True)
            return jnp.where(row_id == 0, one, jnp.where(row_id == 1, two, 0.0)).astype(jnp.int32)

        cnt_r_buf[0] = count_tile(me)
        for o in range(1, 16):
            cnt_s_buf[o] = count_tile(expert_at(o // 4, o % 4))
            count_copy(o, (expert_at(o // 4, o % 4), y, c)).start()

    def fw_copy(o, j, side):
        at = pl.ds(al(o * cap + side * half_cap + j * quarter, quarter), quarter)
        return send(arr.at[at], arr.at[at], fw_s.at[o, j], fw_r.at[o, j], (me, (near, far)[j], c))

    def forward(g):
        for j in range(4):
            o = g * 4 + j

            @pl.when(o > 0)
            def _():
                in_copy(g, j, (me, y, c)).wait_recv()
                fw_copy(o, 0, odd).start()
                fw_copy(o, 1, odd).start()

    def ex_copy(o, j, side):
        src = pl.ds(al(o * cap + side * half_cap + j * quarter, quarter), quarter)
        dst = pl.ds(al(o * half_cap + j * quarter, quarter), quarter)
        return send(part.at[src], yr.at[dst], ex_s.at[o, j], ex_r.at[o, j], (me, (near, far)[j], c))

    def experts_of(g):
        for j in range(4):
            o = g * 4 + j

            @pl.when(o > 0)
            def _():
                fw_copy(o, 0, 1 - odd).wait_recv()
                fw_copy(o, 1, 1 - odd).wait_recv()

        at = pl.ds(al(g * rows, rows), rows)
        inputs = arr[at, :]
        gate = lax.dot_general(inputs, wgu[0:share_width, :], NT, preferred_element_type=jnp.float32)
        up = lax.dot_general(inputs, wgu[share_width:, :], NT, preferred_element_type=jnp.float32)
        act = (gate * jax.nn.sigmoid(glu_alpha * gate) * (up + 1.0)).astype(jnp.bfloat16)
        part[at, :] = jnp.dot(act, wd[...], preferred_element_type=jnp.float32).astype(jnp.bfloat16)
        for j in range(4):
            o = g * 4 + j

            @pl.when(o > 0)
            def _():
                ex_copy(o, 0, 1 - odd).start()
                ex_copy(o, 1, 1 - odd).start()

    def ret_copy(o, device):
        at = pl.ds(al(o * half_cap, half_cap), half_cap)
        return send(half_buf.at[at], ret.at[at], rt_s.at[o], rt_r.at[o], device)

    def give_back(g):
        for j in range(4):
            o = g * 4 + j

            @pl.when(o > 0)
            def _():
                ex_copy(o, 0, odd).wait_recv()
                ex_copy(o, 1, odd).wait_recv()
                own = part[pl.ds(al(o * cap + odd * half_cap, half_cap), half_cap), :]
                at = pl.ds(al(o * half_cap, half_cap), half_cap)
                half_buf[at, :] = (own.astype(jnp.float32) + yr[at, :].astype(jnp.float32)).astype(jnp.bfloat16)
                ret_copy(o, (source_at(g, j), y, c)).start()

    def split(value):
        high = value.astype(jnp.bfloat16)
        return high, (value - high.astype(jnp.float32)).astype(jnp.bfloat16)

    def spread(picker, values):
        high, low = split(picker)
        both = jnp.concatenate([high, low], axis=1)
        wide = lax.dot_general(both, values, TN, preferred_element_type=jnp.float32)
        return wide[:tokens] + wide[tokens:]

    half_id = (lax.broadcasted_iota(jnp.int32, (half_cap, tokens), 0) + odd * half_cap).astype(jnp.float32)

    def combine(g):
        @pl.when(g == 0)
        def _():
            ret[0:half_cap, :] = jnp.zeros((half_cap, width), jnp.bfloat16)
            picker = jnp.where(slots[pl.ds(me, 1), :] == slot_id, shares[pl.ds(me, 1), :], 0.0)
            acc[...] = spread(picker, part[0:cap, :])

        pickers = []
        for j in range(4):
            o = g * 4 + j

            @pl.when(o > 0)
            def _():
                ret_copy(o, (me, y, c)).wait_recv()

            e = expert_at(g, j)
            pickers.append(jnp.where(slots[pl.ds(e, 1), :] == half_id, shares[pl.ds(e, 1), :], 0.0))
        at = pl.ds(al(g * half_rows, half_rows), half_rows)
        acc[...] += spread(jnp.concatenate(pickers, axis=0), ret[at, :])

    load_wgu.wait()
    load_wd.wait()

    def step(i, _):
        @pl.when(i < GROUPS)
        def _():
            forward(i)

        @pl.when(jnp.logical_and(i >= 1, i < GROUPS + 1))
        def _():
            experts_of(i - 1)

        @pl.when(jnp.logical_and(i >= 2, i < GROUPS + 2))
        def _():
            give_back(i - 2)

        @pl.when(i >= 4)
        def _():
            combine(i - 4)

        return 0

    lax.fori_loop(0, GROUPS + 4, step, 0)

    if last:
        for q in range(SIDE):
            rs_send[q] = acc[:, q * share_width : (q + 1) * share_width].astype(jnp.bfloat16)
    else:
        rs_send[...] = acc[...].astype(jnp.bfloat16)
    portion = tokens // SIDE

    def rs_copy(k):
        to = (y + k) % SIDE
        src = rs_send.at[to] if last else rs_send.at[pl.ds(al(to * portion, portion), portion)]
        return send(src, rs_recv.at[k - 1], rs_s.at[k - 1], rs_r.at[k - 1], (me, to, c))

    for k in range(1, SIDE):
        rs_copy(k).start()
    if not last:
        total = cnt_r_buf[0]
        for o in range(1, 16):
            count_copy(o, (me, y, c)).wait_recv()
            total = total + cnt_r_buf[o]
        pair_s_buf[...] = total
        pair = send(pair_s_buf, pair_r_buf, cs.at[0], cr.at[0], (me, y, 1 - c))
        pair.start()
    for k in range(1, SIDE):
        rs_copy(k).wait_recv()
    if last:
        others = rs_recv[0].astype(jnp.float32) + rs_recv[1].astype(jnp.float32) + rs_recv[2].astype(jnp.float32)
        for q in range(SIDE):

            @pl.when(y == q)
            def _():
                cols = slice(q * share_width, (q + 1) * share_width)
                out_ref[...] = (x_ref[:, cols].astype(jnp.float32) + (acc[:, cols] + others)).astype(jnp.bfloat16)
    else:
        mine = pl.ds(al(y * portion, portion), portion)
        others = rs_recv[0].astype(jnp.float32) + rs_recv[1].astype(jnp.float32) + rs_recv[2].astype(jnp.float32)
        gathered[mine, :] = (x_ref[mine, :].astype(jnp.float32) + (acc[mine, :] + others)).astype(jnp.bfloat16)

        def ag_copy(k, owner):
            at = pl.ds(al(owner * portion, portion), portion)
            return send(gathered.at[at], gathered.at[at], ag_s.at[k - 1], ag_r.at[k - 1], (me, (y + k) % SIDE, c))

        for k in range(1, SIDE):
            ag_copy(k, y).start()
        pair.wait_recv()
        load_ref[...] = pair_s_buf[...] + pair_r_buf[...]
        for k in range(1, SIDE):
            ag_copy(k, (y - k + SIDE) % SIDE).wait_recv()
        out_ref[...] = gathered[...]

    def drain(o, _):
        @pl.when(o > 0)
        def _():
            in_copy(o // 4, o % 4, (me, y, c)).wait_send()
            fw_copy(o, 0, odd).wait_send()
            fw_copy(o, 1, odd).wait_send()
            ex_copy(o, 0, 1 - odd).wait_send()
            ex_copy(o, 1, 1 - odd).wait_send()
            ret_copy(o, (me, y, c)).wait_send()
            if not last:
                count_copy(o, (me, y, c)).wait_send()

        return 0

    lax.fori_loop(0, 16, drain, 0)
    for k in range(1, SIDE):
        rs_copy(k).wait_send()
        if not last:
            ag_copy(k, y).wait_send()
    if not last:
        pair.wait_send()


def layer(last, x, routes, shares, gains, gate_up, down, more_routes=None):
    tokens, width = x.shape
    ex = lax.axis_size("ex")
    top = routes.shape[1]
    share_width = down.shape[1]
    cap = 2 * tokens * top // ex
    slots = ex * cap
    bf, f32, i32 = jnp.bfloat16, jnp.float32, jnp.int32
    wgu = jnp.transpose(gate_up[0], (1, 2, 0)).reshape(2 * share_width, width)
    wd = down[0]
    vmem = pl.BlockSpec(memory_space=pltpu.VMEM)
    hbm = pl.BlockSpec(memory_space=pl.ANY)
    small = [x, routes.T] + ([] if last else [more_routes.T]) + [shares.T, gains.reshape(1, width)]
    rs_shape = (SIDE, tokens, share_width) if last else (tokens, width)
    rr_shape = (SIDE - 1, tokens, share_width) if last else (SIDE - 1, tokens // SIDE, width)
    dma = pltpu.SemaphoreType.DMA
    scratch = [
        pltpu.VMEM((2 * share_width, width), bf),
        pltpu.VMEM((share_width, width), bf),
        pltpu.VMEM((tokens, width), bf),
        pltpu.VMEM((ex, tokens), f32),
        pltpu.VMEM((ex, tokens), f32),
        pltpu.VMEM((slots, width), bf),
        pltpu.VMEM((slots, width), bf),
        pltpu.VMEM((slots, width), bf),
        pltpu.VMEM((slots // 2, width), bf),
        pltpu.VMEM((slots // 2, width), bf),
        pltpu.VMEM((slots // 2, width), bf),
        pltpu.VMEM((tokens, width), f32),
        pltpu.VMEM(rs_shape, bf),
        pltpu.VMEM(rr_shape, bf),
        dma((2,)),
        dma((16,)), dma((16,)),
        dma((16, 2)), dma((16, 2)),
        dma((16, 2)), dma((16, 2)),
        dma((16,)), dma((16,)),
        dma((3,)), dma((3,)),
    ]
    out_shape = [jax.ShapeDtypeStruct((tokens, share_width if last else width), bf)]
    if not last:
        out_shape.append(jax.ShapeDtypeStruct((8, 128), i32))
        scratch += [
            pltpu.VMEM((2, ex, tokens), f32),
            pltpu.VMEM((16, 8, 128), i32),
            pltpu.VMEM((16, 8, 128), i32),
            pltpu.VMEM((8, 128), i32),
            pltpu.VMEM((8, 128), i32),
            pltpu.VMEM((tokens, width), bf),
            dma((16,)), dma((16,)), dma((3,)), dma((3,)),
        ]
    return pl.pallas_call(
        functools.partial(layer_kernel, last, cap),
        name="layer_two" if last else "layer_one",
        out_shape=out_shape,
        in_specs=[vmem] * len(small) + [hbm, hbm],
        out_specs=[vmem] * len(out_shape),
        scratch_shapes=scratch,
        compiler_params=pltpu.CompilerParams(
            collective_id=1 if last else 0, has_side_effects=True, vmem_limit_bytes=64 * 1024 * 1024 - 65536
        ),
    )(*small, wgu, wd)


def body(
    tokens, route_one, route_two, share_one, share_two, gain_one, gain_two, gate_up_one, down_one, gate_up_two, down_two
):
    stream, load = layer(False, tokens, route_one, share_one, gain_one, gate_up_one, down_one, route_two)
    (mixed,) = layer(True, stream, route_two, share_two, gain_two, gate_up_two, down_two)
    return mixed, load[0:2, 0:1]


def solution(mesh):
    in_specs = (
        P(("ex", "dp"), None),
        P(("ex", "dp"), None),
        P(("ex", "dp"), None),
        P(("ex", "dp"), None),
        P(("ex", "dp"), None),
        P(),
        P(),
        P("ex", None, None, "tp"),
        P("ex", "tp", None),
        P("ex", None, None, "tp"),
        P("ex", "tp", None),
    )
    out_specs = (P(("ex", "dp"), "tp"), P(None, "ex"))
    return jax.shard_map(body, mesh=mesh, in_specs=in_specs, out_specs=out_specs, check_vma=False)
```

```python
import functools

import jax
import jax.numpy as jnp
from jax import lax
from jax.experimental import pallas as pl
from jax.experimental.pallas import tpu as pltpu
from jax.sharding import PartitionSpec as P

MESH = pl.DeviceIdType.MESH
norm_eps = 1e-05
glu_alpha = 1.702
SIDE = 4
GROUPS = 4
OFFSETS = (
    (0, 0), (2, 2), (1, 1), (3, 3),
    (1, 3), (3, 1), (2, 1), (2, 3),
    (1, 2), (3, 2), (2, 0), (0, 2),
    (1, 0), (3, 0), (0, 1), (0, 3),
)
MODES_IN = "DQHHHHQQHHHHDDDD"
MODES_OUT = "DQHHHHQQHHHHDDDD"
COLUMNS = 1536
NT = (((1,), (1,)), ((), ()))
TN = (((0,), (0,)), ((), ()))
BF, F32, I32 = jnp.bfloat16, jnp.float32, jnp.int32


def al(v, m):
    return pl.multiple_of(v, m)


def moe_kernel(cap, *refs):
    (
        xt_ref, rt1_ref, rt2_ref, st1_ref, st2_ref, gain1_ref, gain2_ref, wgu1, wd1, wgu2, wd2, out_ref, load_ref,
        wgu, wd, x_buf, normed, hits, slots, shares, pk, arr, part, yr, half_buf, ret, acc, rs1_send, rs1_recv,
        rs2_send, rs2_recv, cnt_s_buf, cnt_r_buf, pair_s_buf, pair_r_buf,
        gains, w_sem, in_s, in_r, fw_s, fw_r, ex_s, ex_r, rt_s, rt_r, rs_s, rs_r, ag_s, ag_r, cs, cr,
    ) = refs
    width, tokens = xt_ref.shape
    share_width = wd.shape[0]
    half_cap = cap // 2
    quarter = cap // 4
    rows = 4 * cap
    portion = tokens // SIDE
    parts = ((0, COLUMNS), (COLUMNS, width - COLUMNS))
    cols = tuple(pl.ds(*p) for p in parts)

    me = lax.axis_index("ex")
    y = lax.axis_index("tp")
    c = lax.axis_index("dp")
    my_x, my_z = me // SIDE, me % SIDE
    odd = y % 2
    near = (y + 1 - 2 * odd + SIDE) % SIDE
    far = (y - 1 + 2 * odd + SIDE) % SIDE
    partners = (near, far, (y + 2) % SIDE)

    def expert_at(o):
        dx, dz = OFFSETS[o]
        return ((my_x + dx) % SIDE) * SIDE + (my_z + dz) % SIDE

    def source_at(o):
        dx, dz = OFFSETS[o]
        return ((my_x - dx + SIDE) % SIDE) * SIDE + (my_z - dz + SIDE) % SIDE

    def send(src, dst, s_sem, r_sem, device):
        return pltpu.make_async_remote_copy(
            src_ref=src, dst_ref=dst, send_sem=s_sem, recv_sem=r_sem, device_id=device, device_id_type=MESH
        )

    barrier = pltpu.get_barrier_semaphore()
    for o in range(1, 16):
        pl.semaphore_signal(barrier, inc=1, device_id=(expert_at(o), y, c), device_id_type=MESH)
    for k in range(1, SIDE):
        pl.semaphore_signal(barrier, inc=1, device_id=(me, (y + k) % SIDE, c), device_id_type=MESH)
    pl.semaphore_signal(barrier, inc=1, device_id=(me, y, 1 - c), device_id_type=MESH)

    def weights(gu, down):
        return pltpu.make_async_copy(gu, wgu, w_sem.at[0]), pltpu.make_async_copy(down, wd, w_sem.at[1])

    for load in weights(wgu1, wd1):
        load.start()

    experts = slots.shape[1]
    expert_id = lax.broadcasted_iota(I32, (experts, tokens), 0)
    before = lax.broadcasted_iota(I32, (tokens, tokens), 0) < lax.broadcasted_iota(I32, (tokens, tokens), 1)
    before = jnp.where(before, 1.0, 0.0).astype(BF)
    for level, (rt_ref, st_ref) in enumerate(((rt1_ref, st1_ref), (rt2_ref, st2_ref))):
        table = rt_ref[...]
        hit = jnp.zeros((experts, tokens), F32)
        weight = jnp.zeros((experts, tokens), F32)
        for k in range(table.shape[0]):
            same = table[k : k + 1, :] == expert_id
            hit = hit + jnp.where(same, 1.0, 0.0)
            weight = weight + jnp.where(same, st_ref[k : k + 1, :], 0.0)
        rank = jnp.dot(hit.astype(BF), before, preferred_element_type=F32)
        hits[level] = hit
        slots[level] = jnp.where(hit > 0.5, rank, -1.0)
        shares[level] = weight

    lane_id = lax.broadcasted_iota(I32, (8, 128), 1)

    def count_tile(e):
        one = jnp.sum(hits[0, pl.ds(e, 1), :], axis=1, keepdims=True)
        two = jnp.sum(hits[1, pl.ds(e, 1), :], axis=1, keepdims=True)
        return jnp.where(lane_id == 0, one, jnp.where(lane_id == 1, two, 0.0)).astype(I32)

    def count_copy(o, device):
        return send(cnt_s_buf.at[o], cnt_r_buf.at[o], cs.at[o], cr.at[o], device)

    pair = send(pair_s_buf, pair_r_buf, cs.at[0], cr.at[0], (me, y, 1 - c))

    for k in range(0, width, 128):
        wide = min(128, width - k)
        x_buf[:, k : k + wide] = xt_ref[k : k + wide, :].astype(F32).T.astype(BF)

    gains[0] = gain1_ref[...].reshape(1, width)
    gains[1] = gain2_ref[...].reshape(1, width)
    slot_id = lax.broadcasted_iota(I32, (cap, tokens), 0).astype(F32)
    half_id = (lax.broadcasted_iota(I32, (half_cap, tokens), 0) + odd * half_cap).astype(F32)
    quarter_id = (lax.broadcasted_iota(I32, (quarter, tokens), 0) + y * quarter).astype(F32)
    kept = {"D": cap, "H": half_cap, "Q": quarter}
    ids = {"D": slot_id, "H": half_id, "Q": quarter_id}
    swaps = {"D": 0, "H": 2, "Q": 3}

    def split(value):
        high = value.astype(BF)
        return high, (value - high.astype(F32)).astype(BF)

    def spread(picker, values):
        high, low = split(picker)
        both = jnp.concatenate([high, low], axis=1)
        wide = lax.dot_general(both, values, TN, preferred_element_type=F32)
        return wide[:tokens] + wide[tokens:]

    def own_rows(mode, o):
        start = {"D": 0, "H": odd * half_cap, "Q": y * quarter}[mode]
        return pl.ds(al(o * cap + start, kept[mode]), kept[mode])

    def swap_rows(mode, o, j, mine):
        if mode == "H":
            return pl.ds(al(o * cap + (odd if mine else 1 - odd) * half_cap + j * quarter, quarter), quarter)
        return pl.ds(al(o * cap + (y if mine else partners[j]) * quarter, quarter), quarter)

    def in_copy(o, device):
        at = own_rows(MODES_IN[o], o)
        return send(pk.at[at], arr.at[at], in_s.at[o], in_r.at[o], device)

    def fw_copy(o, j, mine):
        at = swap_rows(MODES_IN[o], o, j, mine)
        return send(arr.at[at], arr.at[at], fw_s.at[o, j], fw_r.at[o, j], (me, partners[j], c))

    def ex_rows(o, j):
        return pl.ds((o * 3 + j) * quarter, quarter)

    def ex_copy(o, j, h):
        src = swap_rows(MODES_OUT[o], o, j, False)
        return send(
            part.at[src, cols[h]], yr.at[ex_rows(o, j), cols[h]], ex_s.at[o, j, h], ex_r.at[o, j, h], (me, partners[j], c)
        )

    def ret_rows(o):
        return pl.ds(o * cap, kept[MODES_OUT[o]])

    def ret_copy(o, h, device):
        if MODES_OUT[o] == "D":
            src = part.at[pl.ds(o * cap, cap), cols[h]]
        else:
            src = half_buf.at[pl.ds(o * half_cap, kept[MODES_OUT[o]]), cols[h]]
        return send(src, ret.at[ret_rows(o), cols[h]], rt_s.at[o, h], rt_r.at[o, h], device)

    def group(g):
        return range(4 * g, 4 * g + 4)

    def forward(g):
        for o in group(g):
            if o > 0:
                in_copy(o, (me, y, c)).wait_recv()
                for j in range(swaps[MODES_IN[o]]):
                    fw_copy(o, j, True).start()

    def experts_of(g):
        for o in group(g):
            for j in range(swaps[MODES_IN[o]]):
                fw_copy(o, j, False).wait_recv()
        at = slice(g * rows, (g + 1) * rows)
        inputs = arr[at, :]
        gate = lax.dot_general(inputs, wgu[0:share_width, :], NT, preferred_element_type=F32)
        up = lax.dot_general(inputs, wgu[share_width:, :], NT, preferred_element_type=F32)
        act = (gate * jax.nn.sigmoid(glu_alpha * gate) * (up + 1.0)).astype(BF)
        part[at, :] = jnp.dot(act, wd[...], preferred_element_type=F32).astype(BF)
        for o in group(g):
            for j in range(swaps[MODES_IN[o]]):
                fw_copy(o, j, True).wait_send()
        for h in range(2):
            for o in group(g):
                if o > 0 and MODES_OUT[o] == "D":
                    ret_copy(o, h, (source_at(o), y, c)).start()
                for j in range(swaps[MODES_OUT[o]]):
                    ex_copy(o, j, h).start()

    def give_back(g, h):
        for o in group(g):
            mode = MODES_OUT[o]
            if mode == "D":
                continue
            total = part[own_rows(mode, o), cols[h]].astype(F32)
            got = []
            for j in range(swaps[mode]):
                ex_copy(o, j, h).wait_recv()
                got.append(yr[ex_rows(o, j), cols[h]].astype(F32))
            if mode == "H":
                total = total + jnp.concatenate(got, axis=0)
            else:
                total = total + got[0] + got[1] + got[2]
            half_buf[pl.ds(o * half_cap, kept[mode]), cols[h]] = total.astype(BF)
            ret_copy(o, h, (source_at(o), y, c)).start()

    def combine(slot, share, g, h):
        pickers, values = [], []
        for o in group(g):
            e = expert_at(o)
            if o == 0:
                values.append(part[0:cap, cols[h]])
            else:
                ret_copy(o, h, (me, y, c)).wait_recv()
                values.append(ret[ret_rows(o), cols[h]])
            pickers.append(jnp.where(slot[pl.ds(e, 1), :] == ids[MODES_OUT[o]], share[pl.ds(e, 1), :], 0.0))
        total = spread(jnp.concatenate(pickers, axis=0), jnp.concatenate(values, axis=0))
        if g == 0:
            acc[:, cols[h]] = total
        else:
            acc[:, cols[h]] += total

    def rs1_copy(k, h):
        to = (y + k) % SIDE
        src = rs1_send.at[pl.ds(al(to * portion, portion), portion), cols[h]]
        return send(src, rs1_recv.at[k - 1, :, cols[h]], rs_s.at[h, k - 1], rs_r.at[h, k - 1], (me, to, c))

    def rs2_copy(k, to):
        return send(rs2_send.at[to], rs2_recv.at[k - 1], rs_s.at[2, k - 1], rs_r.at[2, k - 1], (me, to, c))

    def ag_copy(k, owner, h):
        at = pl.ds(al(owner * portion, portion), portion)
        there = x_buf.at[at, cols[h]]
        return send(there, there, ag_s.at[h, k - 1], ag_r.at[h, k - 1], (me, (y + k) % SIDE, c))

    def sent_all():
        for o in range(1, 16):
            in_copy(o, (me, y, c)).wait_send()
            for h in range(2):
                for j in range(swaps[MODES_OUT[o]]):
                    ex_copy(o, j, h).wait_send()
                ret_copy(o, h, (me, y, c)).wait_send()

    def rs_start(first, h):
        @pl.when(first)
        def _():
            rs1_send[:, cols[h]] = acc[:, cols[h]].astype(BF)
            for k in range(1, SIDE):
                rs1_copy(k, h).start()

        @pl.when(jnp.logical_not(first))
        def _():
            for q in (2 * h, 2 * h + 1):
                rs2_send[q] = acc[:, q * share_width : (q + 1) * share_width].astype(BF)

                @pl.when(y != q)
                def _():
                    rs2_copy((q - y + SIDE) % SIDE, q).start()

    def layer(level, _):
        first = level == 0
        slot = slots.at[level]
        share = shares.at[level]

        gain = gains[level]
        for r in range(0, tokens, 16):
            v = x_buf[r : r + 16, :].astype(F32)
            inverse = lax.rsqrt(jnp.mean(v * v, axis=1, keepdims=True) + norm_eps)
            normed[r : r + 16, :] = (v * inverse * gain).astype(BF)

        @pl.when(first)
        def _():
            pl.semaphore_wait(barrier, 19)

        for g in range(GROUPS):
            chooser = jnp.concatenate(
                [jnp.where(slot[pl.ds(expert_at(o), 1), :] == slot_id, 1.0, 0.0) for o in group(g)], axis=0
            ).astype(BF)
            packed = jnp.dot(chooser, normed[...], preferred_element_type=F32).astype(BF)
            pk[g * rows : (g + 1) * rows, :] = packed
            if g == 0:
                arr[0:cap, :] = packed[0:cap]
            for o in group(g):
                if o > 0:
                    in_copy(o, (expert_at(o), y, c)).start()

        @pl.when(first)
        def _():
            cnt_r_buf[0] = count_tile(me)
            for o in range(1, 16):
                cnt_s_buf[o] = count_tile(expert_at(o))
                count_copy(o, (expert_at(o), y, c)).start()

        for load in weights(wgu1, wd1):
            load.wait()
        forward(0)
        forward(1)
        experts_of(0)
        forward(2)
        experts_of(1)
        forward(3)
        give_back(0, 0)
        give_back(0, 1)
        experts_of(3)
        experts_of(2)

        @pl.when(first)
        def _():
            for load in weights(wgu2, wd2):
                load.start()

        give_back(1, 0)
        give_back(1, 1)
        combine(slot, share, 0, 0)
        give_back(2, 0)
        combine(slot, share, 3, 0)
        combine(slot, share, 1, 0)
        give_back(2, 1)
        combine(slot, share, 2, 0)
        rs_start(first, 0)
        combine(slot, share, 0, 1)
        combine(slot, share, 3, 1)
        combine(slot, share, 1, 1)
        combine(slot, share, 2, 1)
        rs_start(first, 1)

        @pl.when(first)
        def _():
            mine = pl.ds(al(y * portion, portion), portion)
            for h in range(2):
                for k in range(1, SIDE):
                    rs1_copy(k, h).wait_recv()
                others = rs1_recv[0, :, cols[h]].astype(F32)
                for k in range(1, SIDE - 1):
                    others = others + rs1_recv[k, :, cols[h]].astype(F32)
                x_buf[mine, cols[h]] = (x_buf[mine, cols[h]].astype(F32) + (acc[mine, cols[h]] + others)).astype(BF)
                for k in range(1, SIDE):
                    ag_copy(k, y, h).start()
                if h == 0:
                    total = cnt_r_buf[0]
                    for o in range(1, 16):
                        count_copy(o, (me, y, c)).wait_recv()
                        total = total + cnt_r_buf[o]
                    pair_s_buf[...] = total
                    pair.start()
                    sent_all()
                    for o in range(1, 16):
                        count_copy(o, (me, y, c)).wait_send()
            pair.wait_recv()
            load_ref[...] = (pair_s_buf[...] + pair_r_buf[...])[0:1, 0:2]
            pair.wait_send()
            for h in range(2):
                for k in range(1, SIDE):
                    rs1_copy(k, h).wait_send()
                    ag_copy(k, (y - k + SIDE) % SIDE, h).wait_recv()
            for h in range(2):
                for k in range(1, SIDE):
                    ag_copy(k, y, h).wait_send()

        @pl.when(level == 1)
        def _():
            sent_all()
            for k in range(1, SIDE):
                rs2_copy(k, y).wait_recv()
            others = rs2_recv[0].astype(F32) + rs2_recv[1].astype(F32) + rs2_recv[2].astype(F32)
            for q in range(SIDE):

                @pl.when(y == q)
                def _():
                    own = slice(q * share_width, (q + 1) * share_width)
                    out_ref[...] = (x_buf[:, own].astype(F32) + (acc[:, own] + others)).T.astype(BF)

            for k in range(1, SIDE):
                rs2_copy(k, (y + k) % SIDE).wait_send()

        return 0

    lax.fori_loop(0, 2, layer, 0)


def body(
    tokens, route_one, route_two, share_one, share_two, gain_one, gain_two, gate_up_one, down_one, gate_up_two, down_two
):
    count, width = tokens.shape
    ex = lax.axis_size("ex")
    top = route_one.shape[1]
    share_width = down_one.shape[1]
    cap = 2 * count * top // ex
    total = ex * cap
    vmem = pl.BlockSpec(memory_space=pltpu.VMEM)
    hbm = pl.BlockSpec(memory_space=pl.ANY)
    dma = pltpu.SemaphoreType.DMA

    def flat(gate_up):
        return jnp.transpose(gate_up[0], (1, 2, 0)).reshape(2 * share_width, width)

    mixed, load = pl.pallas_call(
        functools.partial(moe_kernel, cap),
        name="two_layers",
        out_shape=[jax.ShapeDtypeStruct((share_width, count), BF), jax.ShapeDtypeStruct((1, 2), I32)],
        in_specs=[vmem] * 7 + [hbm] * 4,
        out_specs=[vmem] * 2,
        scratch_shapes=[
            pltpu.VMEM((2 * share_width, width), BF),
            pltpu.VMEM((share_width, width), BF),
            pltpu.VMEM((count, width), BF),
            pltpu.VMEM((count, width), BF),
            pltpu.VMEM((2, ex, count), F32),
            pltpu.VMEM((2, ex, count), F32),
            pltpu.VMEM((2, ex, count), F32),
            pltpu.VMEM((total, width), BF),
            pltpu.VMEM((total, width), BF),
            pltpu.VMEM((total, width), BF),
            pltpu.VMEM((total * 3 // 4, width), BF),
            pltpu.VMEM((total // 2, width), BF),
            pltpu.VMEM((total, width), BF),
            pltpu.VMEM((count, width), F32),
            pltpu.VMEM((count, width), BF),
            pltpu.VMEM((SIDE - 1, count // SIDE, width), BF),
            pltpu.VMEM((SIDE, count, share_width), BF),
            pltpu.VMEM((SIDE - 1, count, share_width), BF),
            pltpu.VMEM((16, 8, 128), I32),
            pltpu.VMEM((16, 8, 128), I32),
            pltpu.VMEM((8, 128), I32),
            pltpu.VMEM((8, 128), I32),
            pltpu.VMEM((2, 1, width), F32),
            dma((2,)),
            dma((16,)), dma((16,)),
            dma((16, 3)), dma((16, 3)),
            dma((16, 3, 2)), dma((16, 3, 2)),
            dma((16, 2)), dma((16, 2)),
            dma((3, 3)), dma((3, 3)),
            dma((2, 3)), dma((2, 3)),
            dma((16,)), dma((16,)),
        ],
        compiler_params=pltpu.CompilerParams(
            collective_id=0, has_side_effects=True, vmem_limit_bytes=64 * 1024 * 1024 - 65536
        ),
    )(
        tokens.T, route_one.T, route_two.T, share_one.T, share_two.T, gain_one, gain_two,
        flat(gate_up_one), down_one[0], flat(gate_up_two), down_two[0],
    )
    return mixed.T, load.T


def solution(mesh):
    in_specs = (
        P(("ex", "dp"), None),
        P(("ex", "dp"), None),
        P(("ex", "dp"), None),
        P(("ex", "dp"), None),
        P(("ex", "dp"), None),
        P(),
        P(),
        P("ex", None, None, "tp"),
        P("ex", "tp", None),
        P("ex", None, None, "tp"),
        P("ex", "tp", None),
    )
    out_specs = (P(("ex", "dp"), "tp"), P(None, "ex"))
    return jax.shard_map(body, mesh=mesh, in_specs=in_specs, out_specs=out_specs, check_vma=False)
```

```python
import functools

import jax
import jax.numpy as jnp
from jax import lax
from jax.experimental import pallas as pl
from jax.experimental.pallas import tpu as pltpu
from jax.sharding import PartitionSpec as P

MESH = pl.DeviceIdType.MESH
norm_eps = 1e-05
glu_alpha = 1.702
SIDE = 4
GROUPS = 4
OFFSETS = (
    (0, 0), (2, 2), (1, 1), (3, 3),
    (1, 3), (3, 1), (2, 1), (2, 3),
    (1, 2), (3, 2), (2, 0), (0, 2),
    (1, 0), (3, 0), (0, 1), (0, 3),
)
MODES_IN = "DQHHHHQQHHHHDDDD"
MODES_OUT = "DQHHHHQQQQDDDDDD"
COLUMNS = 2048
NT = (((1,), (1,)), ((), ()))
TN = (((0,), (0,)), ((), ()))
BF, F32, I32 = jnp.bfloat16, jnp.float32, jnp.int32


def al(v, m):
    return pl.multiple_of(v, m)


def moe_kernel(cap, *refs):
    (
        xt_ref, rt1_ref, rt2_ref, st1_ref, st2_ref, gain1_ref, gain2_ref, wgu1, wd1, wgu2, wd2, out_ref, load_ref,
        wgu, wd, x_buf, normed, hits, slots, shares, pk, arr, part, yr, half_buf, ret, acc, rs1_send, rs1_recv,
        rs2_send, rs2_recv, cnt_s_buf, cnt_r_buf, pair_s_buf, pair_r_buf,
        gains, w_sem, in_s, in_r, fw_s, fw_r, ex_s, ex_r, rt_s, rt_r, rs_s, rs_r, ag_s, ag_r, cs, cr,
    ) = refs
    width, tokens = xt_ref.shape
    share_width = wd.shape[0]
    half_cap = cap // 2
    quarter = cap // 4
    rows = 4 * cap
    portion = tokens // SIDE
    parts = ((0, COLUMNS), (COLUMNS, width - COLUMNS))
    cols = tuple(pl.ds(*p) for p in parts)

    me = lax.axis_index("ex")
    y = lax.axis_index("tp")
    c = lax.axis_index("dp")
    my_x, my_z = me // SIDE, me % SIDE
    odd = y % 2
    near = (y + 1 - 2 * odd + SIDE) % SIDE
    far = (y - 1 + 2 * odd + SIDE) % SIDE
    partners = (near, far, (y + 2) % SIDE)

    def expert_at(o):
        dx, dz = OFFSETS[o]
        return ((my_x + dx) % SIDE) * SIDE + (my_z + dz) % SIDE

    def source_at(o):
        dx, dz = OFFSETS[o]
        return ((my_x - dx + SIDE) % SIDE) * SIDE + (my_z - dz + SIDE) % SIDE

    def send(src, dst, s_sem, r_sem, device):
        return pltpu.make_async_remote_copy(
            src_ref=src, dst_ref=dst, send_sem=s_sem, recv_sem=r_sem, device_id=device, device_id_type=MESH
        )

    barrier = pltpu.get_barrier_semaphore()
    for o in range(1, 16):
        pl.semaphore_signal(barrier, inc=1, device_id=(expert_at(o), y, c), device_id_type=MESH)
    for k in range(1, SIDE):
        pl.semaphore_signal(barrier, inc=1, device_id=(me, (y + k) % SIDE, c), device_id_type=MESH)
    pl.semaphore_signal(barrier, inc=1, device_id=(me, y, 1 - c), device_id_type=MESH)

    def weights(gu, down):
        return pltpu.make_async_copy(gu, wgu, w_sem.at[0]), pltpu.make_async_copy(down, wd, w_sem.at[1])

    for load in weights(wgu1, wd1):
        load.start()

    experts = slots.shape[1]
    expert_id = lax.broadcasted_iota(I32, (experts, tokens), 0)
    before = lax.broadcasted_iota(I32, (tokens, tokens), 0) < lax.broadcasted_iota(I32, (tokens, tokens), 1)
    before = jnp.where(before, 1.0, 0.0).astype(BF)
    for level, (rt_ref, st_ref) in enumerate(((rt1_ref, st1_ref), (rt2_ref, st2_ref))):
        table = rt_ref[...]
        hit = jnp.zeros((experts, tokens), F32)
        weight = jnp.zeros((experts, tokens), F32)
        for k in range(table.shape[0]):
            same = table[k : k + 1, :] == expert_id
            hit = hit + jnp.where(same, 1.0, 0.0)
            weight = weight + jnp.where(same, st_ref[k : k + 1, :], 0.0)
        rank = jnp.dot(hit.astype(BF), before, preferred_element_type=F32)
        hits[level] = hit
        slots[level] = jnp.where(hit > 0.5, rank, -1.0)
        shares[level] = weight

    lane_id = lax.broadcasted_iota(I32, (8, 128), 1)

    def count_tile(e):
        one = jnp.sum(hits[0, pl.ds(e, 1), :], axis=1, keepdims=True)
        two = jnp.sum(hits[1, pl.ds(e, 1), :], axis=1, keepdims=True)
        return jnp.where(lane_id == 0, one, jnp.where(lane_id == 1, two, 0.0)).astype(I32)

    def count_copy(o, device):
        return send(cnt_s_buf.at[o], cnt_r_buf.at[o], cs.at[o], cr.at[o], device)

    pair = send(pair_s_buf, pair_r_buf, cs.at[0], cr.at[0], (me, y, 1 - c))

    for k in range(0, width, 128):
        wide = min(128, width - k)
        x_buf[:, k : k + wide] = xt_ref[k : k + wide, :].astype(F32).T.astype(BF)

    gains[0] = gain1_ref[...].reshape(1, width)
    gains[1] = gain2_ref[...].reshape(1, width)
    slot_id = lax.broadcasted_iota(I32, (cap, tokens), 0).astype(F32)
    half_id = (lax.broadcasted_iota(I32, (half_cap, tokens), 0) + odd * half_cap).astype(F32)
    quarter_id = (lax.broadcasted_iota(I32, (quarter, tokens), 0) + y * quarter).astype(F32)
    kept = {"D": cap, "H": half_cap, "Q": quarter}
    ids = {"D": slot_id, "H": half_id, "Q": quarter_id}
    swaps = {"D": 0, "H": 2, "Q": 3}

    def split(value):
        high = value.astype(BF)
        return high, (value - high.astype(F32)).astype(BF)

    def spread(picker, values):
        high, low = split(picker)
        both = jnp.concatenate([high, low], axis=1)
        wide = lax.dot_general(both, values, TN, preferred_element_type=F32)
        return wide[:tokens] + wide[tokens:]

    def own_rows(mode, o):
        start = {"D": 0, "H": odd * half_cap, "Q": y * quarter}[mode]
        return pl.ds(al(o * cap + start, kept[mode]), kept[mode])

    def swap_rows(mode, o, j, mine):
        if mode == "H":
            return pl.ds(al(o * cap + (odd if mine else 1 - odd) * half_cap + j * quarter, quarter), quarter)
        return pl.ds(al(o * cap + (y if mine else partners[j]) * quarter, quarter), quarter)

    def in_copy(o, device):
        at = own_rows(MODES_IN[o], o)
        return send(pk.at[at], arr.at[at], in_s.at[o], in_r.at[o], device)

    def fw_copy(o, j, mine):
        at = swap_rows(MODES_IN[o], o, j, mine)
        return send(arr.at[at], arr.at[at], fw_s.at[o, j], fw_r.at[o, j], (me, partners[j], c))

    def ex_rows(o, j):
        return pl.ds((o * 3 + j) * quarter, quarter)

    def ex_copy(o, j, h):
        src = swap_rows(MODES_OUT[o], o, j, False)
        return send(
            part.at[src, cols[h]], yr.at[ex_rows(o, j), cols[h]], ex_s.at[o, j, h], ex_r.at[o, j, h], (me, partners[j], c)
        )

    def ret_rows(o):
        return pl.ds(o * cap, kept[MODES_OUT[o]])

    def ret_copy(o, h, device):
        if MODES_OUT[o] == "D":
            src = part.at[pl.ds(o * cap, cap), cols[h]]
        else:
            src = half_buf.at[pl.ds(o * half_cap, kept[MODES_OUT[o]]), cols[h]]
        return send(src, ret.at[ret_rows(o), cols[h]], rt_s.at[o, h], rt_r.at[o, h], device)

    def group(g):
        return range(4 * g, 4 * g + 4)

    def forward(g):
        for o in group(g):
            if o > 0:
                in_copy(o, (me, y, c)).wait_recv()
                for j in range(swaps[MODES_IN[o]]):
                    fw_copy(o, j, True).start()

    def experts_of(g, then):
        for o in group(g):
            for j in range(swaps[MODES_IN[o]]):
                fw_copy(o, j, False).wait_recv()
        at = slice(g * rows, (g + 1) * rows)
        inputs = arr[at, :]
        gate = lax.dot_general(inputs, wgu[0:share_width, :], NT, preferred_element_type=F32)
        up = lax.dot_general(inputs, wgu[share_width:, :], NT, preferred_element_type=F32)
        act = (gate * jax.nn.sigmoid(glu_alpha * gate) * (up + 1.0)).astype(BF)
        part[at, :] = jnp.dot(act, wd[...], preferred_element_type=F32).astype(BF)
        for o in group(g):
            for j in range(swaps[MODES_IN[o]]):
                fw_copy(o, j, True).wait_send()
        for p, h in then:
            for o in group(p):
                if o > 0 and MODES_OUT[o] == "D":
                    ret_copy(o, h, (source_at(o), y, c)).start()
                for j in range(swaps[MODES_OUT[o]]):
                    ex_copy(o, j, h).start()

    def give_back(g, h):
        for o in group(g):
            mode = MODES_OUT[o]
            if mode == "D":
                continue
            total = part[own_rows(mode, o), cols[h]].astype(F32)
            got = []
            for j in range(swaps[mode]):
                ex_copy(o, j, h).wait_recv()
                got.append(yr[ex_rows(o, j), cols[h]].astype(F32))
            if mode == "H":
                total = total + jnp.concatenate(got, axis=0)
            else:
                total = total + got[0] + got[1] + got[2]
            half_buf[pl.ds(o * half_cap, kept[mode]), cols[h]] = total.astype(BF)
            ret_copy(o, h, (source_at(o), y, c)).start()

    def combine(slot, share, g, h):
        pickers, values = [], []
        for o in group(g):
            e = expert_at(o)
            if o == 0:
                values.append(part[0:cap, cols[h]])
            else:
                ret_copy(o, h, (me, y, c)).wait_recv()
                values.append(ret[ret_rows(o), cols[h]])
            pickers.append(jnp.where(slot[pl.ds(e, 1), :] == ids[MODES_OUT[o]], share[pl.ds(e, 1), :], 0.0))
        total = spread(jnp.concatenate(pickers, axis=0), jnp.concatenate(values, axis=0))
        if g == 0:
            acc[:, cols[h]] = total
        else:
            acc[:, cols[h]] += total

    def rs1_copy(k, h):
        to = (y + k) % SIDE
        src = rs1_send.at[pl.ds(al(to * portion, portion), portion), cols[h]]
        return send(src, rs1_recv.at[k - 1, :, cols[h]], rs_s.at[h, k - 1], rs_r.at[h, k - 1], (me, to, c))

    def rs2_copy(k, to):
        return send(rs2_send.at[to], rs2_recv.at[k - 1], rs_s.at[2, k - 1], rs_r.at[2, k - 1], (me, to, c))

    def ag_copy(k, owner, h):
        at = pl.ds(al(owner * portion, portion), portion)
        there = x_buf.at[at, cols[h]]
        return send(there, there, ag_s.at[h, k - 1], ag_r.at[h, k - 1], (me, (y + k) % SIDE, c))

    def sent_all():
        for o in range(1, 16):
            in_copy(o, (me, y, c)).wait_send()
            for h in range(2):
                for j in range(swaps[MODES_OUT[o]]):
                    ex_copy(o, j, h).wait_send()
                ret_copy(o, h, (me, y, c)).wait_send()

    def rs_start(first, h):
        @pl.when(first)
        def _():
            rs1_send[:, cols[h]] = acc[:, cols[h]].astype(BF)
            for k in range(1, SIDE):
                rs1_copy(k, h).start()

        @pl.when(jnp.logical_not(first))
        def _():
            for q in (2 * h, 2 * h + 1):
                rs2_send[q] = acc[:, q * share_width : (q + 1) * share_width].astype(BF)

                @pl.when(y != q)
                def _():
                    rs2_copy((q - y + SIDE) % SIDE, q).start()

    def summed(h):
        mine = pl.ds(al(y * portion, portion), portion)
        for k in range(1, SIDE):
            rs1_copy(k, h).wait_recv()
        others = rs1_recv[0, :, cols[h]].astype(F32)
        for k in range(1, SIDE - 1):
            others = others + rs1_recv[k, :, cols[h]].astype(F32)
        x_buf[mine, cols[h]] = (x_buf[mine, cols[h]].astype(F32) + (acc[mine, cols[h]] + others)).astype(BF)
        for k in range(1, SIDE):
            ag_copy(k, y, h).start()

    def layer(level, _):
        first = level == 0
        slot = slots.at[level]
        share = shares.at[level]

        gain = gains[level]
        for r in range(0, tokens, 16):
            v = x_buf[r : r + 16, :].astype(F32)
            inverse = lax.rsqrt(jnp.mean(v * v, axis=1, keepdims=True) + norm_eps)
            normed[r : r + 16, :] = (v * inverse * gain).astype(BF)

        @pl.when(first)
        def _():
            pl.semaphore_wait(barrier, 19)

        for g in range(GROUPS):
            chooser = jnp.concatenate(
                [jnp.where(slot[pl.ds(expert_at(o), 1), :] == slot_id, 1.0, 0.0) for o in group(g)], axis=0
            ).astype(BF)
            packed = jnp.dot(chooser, normed[...], preferred_element_type=F32).astype(BF)
            pk[g * rows : (g + 1) * rows, :] = packed
            if g == 0:
                arr[0:cap, :] = packed[0:cap]
            for o in group(g):
                if o > 0:
                    in_copy(o, (expert_at(o), y, c)).start()

        @pl.when(first)
        def _():
            cnt_r_buf[0] = count_tile(me)
            for o in range(1, 16):
                cnt_s_buf[o] = count_tile(expert_at(o))
                count_copy(o, (expert_at(o), y, c)).start()

        for load in weights(wgu1, wd1):
            load.wait()
        forward(0)
        forward(1)
        experts_of(0, ((0, 0), (0, 1)))
        forward(2)
        experts_of(1, ((1, 0),))
        forward(3)
        give_back(0, 0)
        give_back(0, 1)
        experts_of(3, ((3, 0), (3, 1)))
        experts_of(2, ((2, 0), (1, 1), (2, 1)))

        @pl.when(first)
        def _():
            for load in weights(wgu2, wd2):
                load.start()

        give_back(1, 0)
        combine(slot, share, 0, 0)
        give_back(2, 0)
        give_back(1, 1)
        give_back(2, 1)
        combine(slot, share, 3, 0)
        combine(slot, share, 1, 0)
        combine(slot, share, 2, 0)
        rs_start(first, 0)
        combine(slot, share, 0, 1)
        combine(slot, share, 3, 1)
        combine(slot, share, 1, 1)
        combine(slot, share, 2, 1)
        rs_start(first, 1)

        @pl.when(first)
        def _():
            summed(0)
            total = cnt_r_buf[0]
            for o in range(1, 16):
                count_copy(o, (me, y, c)).wait_recv()
                total = total + cnt_r_buf[o]
            pair_s_buf[...] = total
            pair.start()
            sent_all()
            for o in range(1, 16):
                count_copy(o, (me, y, c)).wait_send()
            summed(1)
            pair.wait_recv()
            load_ref[...] = (pair_s_buf[...] + pair_r_buf[...])[0:1, 0:2]
            pair.wait_send()
            for h in range(2):
                for k in range(1, SIDE):
                    rs1_copy(k, h).wait_send()
                    ag_copy(k, (y - k + SIDE) % SIDE, h).wait_recv()
            for h in range(2):
                for k in range(1, SIDE):
                    ag_copy(k, y, h).wait_send()

        @pl.when(level == 1)
        def _():
            sent_all()
            for k in range(1, SIDE):
                rs2_copy(k, y).wait_recv()
            others = rs2_recv[0].astype(F32) + rs2_recv[1].astype(F32) + rs2_recv[2].astype(F32)
            for q in range(SIDE):

                @pl.when(y == q)
                def _():
                    own = slice(q * share_width, (q + 1) * share_width)
                    out_ref[...] = (x_buf[:, own].astype(F32) + (acc[:, own] + others)).T.astype(BF)

            for k in range(1, SIDE):
                rs2_copy(k, (y + k) % SIDE).wait_send()

        return 0

    lax.fori_loop(0, 2, layer, 0)


def body(
    tokens, route_one, route_two, share_one, share_two, gain_one, gain_two, gate_up_one, down_one, gate_up_two, down_two
):
    count, width = tokens.shape
    ex = lax.axis_size("ex")
    top = route_one.shape[1]
    share_width = down_one.shape[1]
    cap = 2 * count * top // ex
    total = ex * cap
    vmem = pl.BlockSpec(memory_space=pltpu.VMEM)
    hbm = pl.BlockSpec(memory_space=pl.ANY)
    dma = pltpu.SemaphoreType.DMA

    def flat(gate_up):
        return jnp.transpose(gate_up[0], (1, 2, 0)).reshape(2 * share_width, width)

    mixed, load = pl.pallas_call(
        functools.partial(moe_kernel, cap),
        name="two_layers",
        out_shape=[jax.ShapeDtypeStruct((share_width, count), BF), jax.ShapeDtypeStruct((1, 2), I32)],
        in_specs=[vmem] * 7 + [hbm] * 4,
        out_specs=[vmem] * 2,
        scratch_shapes=[
            pltpu.VMEM((2 * share_width, width), BF),
            pltpu.VMEM((share_width, width), BF),
            pltpu.VMEM((count, width), BF),
            pltpu.VMEM((count, width), BF),
            pltpu.VMEM((2, ex, count), F32),
            pltpu.VMEM((2, ex, count), F32),
            pltpu.VMEM((2, ex, count), F32),
            pltpu.VMEM((total, width), BF),
            pltpu.VMEM((total, width), BF),
            pltpu.VMEM((total, width), BF),
            pltpu.VMEM((total * 3 // 4, width), BF),
            pltpu.VMEM((total // 2, width), BF),
            pltpu.VMEM((total, width), BF),
            pltpu.VMEM((count, width), F32),
            pltpu.VMEM((count, width), BF),
            pltpu.VMEM((SIDE - 1, count // SIDE, width), BF),
            pltpu.VMEM((SIDE, count, share_width), BF),
            pltpu.VMEM((SIDE - 1, count, share_width), BF),
            pltpu.VMEM((16, 8, 128), I32),
            pltpu.VMEM((16, 8, 128), I32),
            pltpu.VMEM((8, 128), I32),
            pltpu.VMEM((8, 128), I32),
            pltpu.VMEM((2, 1, width), F32),
            dma((2,)),
            dma((16,)), dma((16,)),
            dma((16, 3)), dma((16, 3)),
            dma((16, 3, 2)), dma((16, 3, 2)),
            dma((16, 2)), dma((16, 2)),
            dma((3, 3)), dma((3, 3)),
            dma((2, 3)), dma((2, 3)),
            dma((16,)), dma((16,)),
        ],
        compiler_params=pltpu.CompilerParams(
            collective_id=0, has_side_effects=True, vmem_limit_bytes=64 * 1024 * 1024 - 65536
        ),
    )(
        tokens.T, route_one.T, route_two.T, share_one.T, share_two.T, gain_one, gain_two,
        flat(gate_up_one), down_one[0], flat(gate_up_two), down_two[0],
    )
    return mixed.T, load.T


def solution(mesh):
    in_specs = (
        P(("ex", "dp"), None),
        P(("ex", "dp"), None),
        P(("ex", "dp"), None),
        P(("ex", "dp"), None),
        P(("ex", "dp"), None),
        P(),
        P(),
        P("ex", None, None, "tp"),
        P("ex", "tp", None),
        P("ex", None, None, "tp"),
        P("ex", "tp", None),
    )
    out_specs = (P(("ex", "dp"), "tp"), P(None, "ex"))
    return jax.shard_map(body, mesh=mesh, in_specs=in_specs, out_specs=out_specs, check_vma=False)
```

```python
import functools

import jax
import jax.numpy as jnp
from jax import lax
from jax.experimental import pallas as pl
from jax.experimental.pallas import tpu as pltpu
from jax.sharding import PartitionSpec as P

MESH = pl.DeviceIdType.MESH
norm_eps = 1e-05
glu_alpha = 1.702
SIDE = 4
GROUPS = 4
OFFSETS = (
    (0, 0), (2, 2), (1, 1), (3, 3),
    (1, 3), (3, 1), (2, 1), (2, 3),
    (1, 2), (3, 2), (2, 0), (0, 2),
    (1, 0), (3, 0), (0, 1), (0, 3),
)
MODES_IN = "DQHHHHQQHHHHDDDD"
MODES_OUT = "DQHHHHQQQQDDDDDD"
COLUMNS = 2304
NT = (((1,), (1,)), ((), ()))
TN = (((0,), (0,)), ((), ()))
BF, F32, I32 = jnp.bfloat16, jnp.float32, jnp.int32


def al(v, m):
    return pl.multiple_of(v, m)


def moe_kernel(cap, *refs):
    (
        xt_ref, rt1_ref, rt2_ref, st1_ref, st2_ref, gain1_ref, gain2_ref, wgu1, wd1, wgu2, wd2, out_ref, load_ref,
        wgu, wd, x_buf, normed, hits, slots, shares, pk, arr, part, yr, half_buf, ret, acc, rs1_send, rs1_recv,
        rs2_send, rs2_recv, cnt_s_buf, cnt_r_buf, pair_s_buf, pair_r_buf,
        gains, w_sem, in_s, in_r, fw_s, fw_r, ex_s, ex_r, rt_s, rt_r, rs_s, rs_r, ag_s, ag_r, cs, cr,
    ) = refs
    width, tokens = xt_ref.shape
    share_width = wd.shape[0]
    half_cap = cap // 2
    quarter = cap // 4
    rows = 4 * cap
    portion = tokens // SIDE
    parts = ((0, COLUMNS), (COLUMNS, width - COLUMNS))
    cols = tuple(pl.ds(*p) for p in parts)

    me = lax.axis_index("ex")
    y = lax.axis_index("tp")
    c = lax.axis_index("dp")
    my_x, my_z = me // SIDE, me % SIDE
    odd = y % 2
    near = (y + 1 - 2 * odd + SIDE) % SIDE
    far = (y - 1 + 2 * odd + SIDE) % SIDE
    partners = (near, far, (y + 2) % SIDE)

    def expert_at(o):
        dx, dz = OFFSETS[o]
        return ((my_x + dx) % SIDE) * SIDE + (my_z + dz) % SIDE

    def source_at(o):
        dx, dz = OFFSETS[o]
        return ((my_x - dx + SIDE) % SIDE) * SIDE + (my_z - dz + SIDE) % SIDE

    def send(src, dst, s_sem, r_sem, device):
        return pltpu.make_async_remote_copy(
            src_ref=src, dst_ref=dst, send_sem=s_sem, recv_sem=r_sem, device_id=device, device_id_type=MESH
        )

    barrier = pltpu.get_barrier_semaphore()
    for o in range(1, 16):
        pl.semaphore_signal(barrier, inc=1, device_id=(expert_at(o), y, c), device_id_type=MESH)
    for k in range(1, SIDE):
        pl.semaphore_signal(barrier, inc=1, device_id=(me, (y + k) % SIDE, c), device_id_type=MESH)
    pl.semaphore_signal(barrier, inc=1, device_id=(me, y, 1 - c), device_id_type=MESH)

    def weights(gu, down):
        return pltpu.make_async_copy(gu, wgu, w_sem.at[0]), pltpu.make_async_copy(down, wd, w_sem.at[1])

    for load in weights(wgu1, wd1):
        load.start()

    experts = slots.shape[1]
    expert_id = lax.broadcasted_iota(I32, (experts, tokens), 0)
    before = lax.broadcasted_iota(I32, (tokens, tokens), 0) < lax.broadcasted_iota(I32, (tokens, tokens), 1)
    before = jnp.where(before, 1.0, 0.0).astype(BF)
    for level, (rt_ref, st_ref) in enumerate(((rt1_ref, st1_ref), (rt2_ref, st2_ref))):
        table = rt_ref[...]
        hit = jnp.zeros((experts, tokens), F32)
        weight = jnp.zeros((experts, tokens), F32)
        for k in range(table.shape[0]):
            same = table[k : k + 1, :] == expert_id
            hit = hit + jnp.where(same, 1.0, 0.0)
            weight = weight + jnp.where(same, st_ref[k : k + 1, :], 0.0)
        rank = jnp.dot(hit.astype(BF), before, preferred_element_type=F32)
        hits[level] = hit
        slots[level] = jnp.where(hit > 0.5, rank, -1.0)
        shares[level] = weight

    lane_id = lax.broadcasted_iota(I32, (8, 128), 1)

    def count_tile(e):
        one = jnp.sum(hits[0, pl.ds(e, 1), :], axis=1, keepdims=True)
        two = jnp.sum(hits[1, pl.ds(e, 1), :], axis=1, keepdims=True)
        return jnp.where(lane_id == 0, one, jnp.where(lane_id == 1, two, 0.0)).astype(I32)

    def count_copy(o, device):
        return send(cnt_s_buf.at[o], cnt_r_buf.at[o], cs.at[o], cr.at[o], device)

    pair = send(pair_s_buf, pair_r_buf, cs.at[0], cr.at[0], (me, y, 1 - c))

    for k in range(0, width, 128):
        wide = min(128, width - k)
        x_buf[:, k : k + wide] = xt_ref[k : k + wide, :].astype(F32).T.astype(BF)

    gains[0] = gain1_ref[...].reshape(1, width)
    gains[1] = gain2_ref[...].reshape(1, width)
    slot_id = lax.broadcasted_iota(I32, (cap, tokens), 0).astype(F32)
    half_id = (lax.broadcasted_iota(I32, (half_cap, tokens), 0) + odd * half_cap).astype(F32)
    quarter_id = (lax.broadcasted_iota(I32, (quarter, tokens), 0) + y * quarter).astype(F32)
    kept = {"D": cap, "H": half_cap, "Q": quarter}
    ids = {"D": slot_id, "H": half_id, "Q": quarter_id}
    swaps = {"D": 0, "H": 2, "Q": 3}

    def split(value):
        high = value.astype(BF)
        return high, (value - high.astype(F32)).astype(BF)

    def spread(picker, values):
        high, low = split(picker)
        both = jnp.concatenate([high, low], axis=1)
        wide = lax.dot_general(both, values, TN, preferred_element_type=F32)
        return wide[:tokens] + wide[tokens:]

    def own_rows(mode, o):
        start = {"D": 0, "H": odd * half_cap, "Q": y * quarter}[mode]
        return pl.ds(al(o * cap + start, kept[mode]), kept[mode])

    def swap_rows(mode, o, j, mine):
        if mode == "H":
            return pl.ds(al(o * cap + (odd if mine else 1 - odd) * half_cap + j * quarter, quarter), quarter)
        return pl.ds(al(o * cap + (y if mine else partners[j]) * quarter, quarter), quarter)

    def in_copy(o, device):
        at = own_rows(MODES_IN[o], o)
        return send(pk.at[at], arr.at[at], in_s.at[o], in_r.at[o], device)

    def fw_copy(o, j, mine):
        at = swap_rows(MODES_IN[o], o, j, mine)
        return send(arr.at[at], arr.at[at], fw_s.at[o, j], fw_r.at[o, j], (me, partners[j], c))

    def ex_rows(o, j):
        return pl.ds((o * 3 + j) * quarter, quarter)

    def ex_copy(o, j, h):
        src = swap_rows(MODES_OUT[o], o, j, False)
        return send(
            part.at[src, cols[h]], yr.at[ex_rows(o, j), cols[h]], ex_s.at[o, j, h], ex_r.at[o, j, h], (me, partners[j], c)
        )

    def ret_rows(o):
        return pl.ds(o * cap, kept[MODES_OUT[o]])

    def ret_copy(o, h, device):
        if MODES_OUT[o] == "D":
            src = part.at[pl.ds(o * cap, cap), cols[h]]
        else:
            src = half_buf.at[pl.ds(o * half_cap, kept[MODES_OUT[o]]), cols[h]]
        return send(src, ret.at[ret_rows(o), cols[h]], rt_s.at[o, h], rt_r.at[o, h], device)

    def group(g):
        return range(4 * g, 4 * g + 4)

    def forward(g):
        for o in group(g):
            if o > 0:
                in_copy(o, (me, y, c)).wait_recv()
                for j in range(swaps[MODES_IN[o]]):
                    fw_copy(o, j, True).start()

    def experts_of(g, then):
        for o in group(g):
            for j in range(swaps[MODES_IN[o]]):
                fw_copy(o, j, False).wait_recv()
        at = slice(g * rows, (g + 1) * rows)
        inputs = arr[at, :]
        gate = lax.dot_general(inputs, wgu[0:share_width, :], NT, preferred_element_type=F32)
        up = lax.dot_general(inputs, wgu[share_width:, :], NT, preferred_element_type=F32)
        act = (gate * jax.nn.sigmoid(glu_alpha * gate) * (up + 1.0)).astype(BF)
        part[at, :] = jnp.dot(act, wd[...], preferred_element_type=F32).astype(BF)
        for o in group(g):
            for j in range(swaps[MODES_IN[o]]):
                fw_copy(o, j, True).wait_send()
        for p, h in then:
            for o in group(p):
                if o > 0 and MODES_OUT[o] == "D":
                    ret_copy(o, h, (source_at(o), y, c)).start()
                for j in range(swaps[MODES_OUT[o]]):
                    ex_copy(o, j, h).start()

    def give_back(g, h):
        for o in group(g):
            mode = MODES_OUT[o]
            if mode == "D":
                continue
            total = part[own_rows(mode, o), cols[h]].astype(F32)
            got = []
            for j in range(swaps[mode]):
                ex_copy(o, j, h).wait_recv()
                got.append(yr[ex_rows(o, j), cols[h]].astype(F32))
            if mode == "H":
                total = total + jnp.concatenate(got, axis=0)
            else:
                total = total + got[0] + got[1] + got[2]
            half_buf[pl.ds(o * half_cap, kept[mode]), cols[h]] = total.astype(BF)
            ret_copy(o, h, (source_at(o), y, c)).start()

    def combine(slot, share, g, h):
        pickers, values = [], []
        for o in group(g):
            e = expert_at(o)
            if o == 0:
                values.append(part[0:cap, cols[h]])
            else:
                ret_copy(o, h, (me, y, c)).wait_recv()
                values.append(ret[ret_rows(o), cols[h]])
            pickers.append(jnp.where(slot[pl.ds(e, 1), :] == ids[MODES_OUT[o]], share[pl.ds(e, 1), :], 0.0))
        total = spread(jnp.concatenate(pickers, axis=0), jnp.concatenate(values, axis=0))
        if g == 0:
            acc[:, cols[h]] = total
        else:
            acc[:, cols[h]] += total

    def rs1_copy(k, h):
        to = (y + k) % SIDE
        src = rs1_send.at[pl.ds(al(to * portion, portion), portion), cols[h]]
        return send(src, rs1_recv.at[k - 1, :, cols[h]], rs_s.at[h, k - 1], rs_r.at[h, k - 1], (me, to, c))

    def rs2_copy(k, to):
        return send(rs2_send.at[to], rs2_recv.at[k - 1], rs_s.at[2, k - 1], rs_r.at[2, k - 1], (me, to, c))

    def ag_copy(k, owner, h):
        at = pl.ds(al(owner * portion, portion), portion)
        there = x_buf.at[at, cols[h]]
        return send(there, there, ag_s.at[h, k - 1], ag_r.at[h, k - 1], (me, (y + k) % SIDE, c))

    def sent_all():
        for o in range(1, 16):
            in_copy(o, (me, y, c)).wait_send()
            for h in range(2):
                for j in range(swaps[MODES_OUT[o]]):
                    ex_copy(o, j, h).wait_send()
                ret_copy(o, h, (me, y, c)).wait_send()

    def rs_start(first, h):
        @pl.when(first)
        def _():
            rs1_send[:, cols[h]] = acc[:, cols[h]].astype(BF)
            for k in range(1, SIDE):
                rs1_copy(k, h).start()

        @pl.when(jnp.logical_not(first))
        def _():
            for q in ((0, 1, 2), (3,))[h]:
                rs2_send[q] = acc[:, q * share_width : (q + 1) * share_width].astype(BF)

                @pl.when(y != q)
                def _():
                    rs2_copy((q - y + SIDE) % SIDE, q).start()

    def summed(h):
        mine = pl.ds(al(y * portion, portion), portion)
        for k in range(1, SIDE):
            rs1_copy(k, h).wait_recv()
        others = rs1_recv[0, :, cols[h]].astype(F32)
        for k in range(1, SIDE - 1):
            others = others + rs1_recv[k, :, cols[h]].astype(F32)
        x_buf[mine, cols[h]] = (x_buf[mine, cols[h]].astype(F32) + (acc[mine, cols[h]] + others)).astype(BF)
        for k in range(1, SIDE):
            ag_copy(k, y, h).start()

    def layer(level, _):
        first = level == 0
        slot = slots.at[level]
        share = shares.at[level]

        gain = gains[level]
        for r in range(0, tokens, 16):
            v = x_buf[r : r + 16, :].astype(F32)
            inverse = lax.rsqrt(jnp.mean(v * v, axis=1, keepdims=True) + norm_eps)
            normed[r : r + 16, :] = (v * inverse * gain).astype(BF)

        for g in range(GROUPS):
            chooser = jnp.concatenate(
                [jnp.where(slot[pl.ds(expert_at(o), 1), :] == slot_id, 1.0, 0.0) for o in group(g)], axis=0
            ).astype(BF)
            packed = jnp.dot(chooser, normed[...], preferred_element_type=F32).astype(BF)
            pk[g * rows : (g + 1) * rows, :] = packed
            if g == 0:
                arr[0:cap, :] = packed[0:cap]

                @pl.when(first)
                def _():
                    pl.semaphore_wait(barrier, 19)

            for o in group(g):
                if o > 0:
                    in_copy(o, (expert_at(o), y, c)).start()

        @pl.when(first)
        def _():
            cnt_r_buf[0] = count_tile(me)
            for o in range(1, 16):
                cnt_s_buf[o] = count_tile(expert_at(o))
                count_copy(o, (expert_at(o), y, c)).start()

        for load in weights(wgu1, wd1):
            load.wait()
        forward(0)
        forward(1)
        experts_of(0, ((0, 0), (0, 1)))
        forward(2)
        experts_of(1, ((1, 0),))
        forward(3)
        give_back(0, 0)
        give_back(0, 1)
        experts_of(3, ((3, 0), (3, 1)))
        experts_of(2, ((2, 0), (1, 1), (2, 1)))

        @pl.when(first)
        def _():
            for load in weights(wgu2, wd2):
                load.start()

        give_back(1, 0)
        combine(slot, share, 0, 0)
        give_back(2, 0)
        give_back(1, 1)
        give_back(2, 1)
        combine(slot, share, 3, 0)
        combine(slot, share, 1, 0)
        combine(slot, share, 2, 0)
        rs_start(first, 0)
        combine(slot, share, 0, 1)
        combine(slot, share, 3, 1)
        combine(slot, share, 1, 1)
        combine(slot, share, 2, 1)
        rs_start(first, 1)

        @pl.when(first)
        def _():
            summed(0)
            total = cnt_r_buf[0]
            for o in range(1, 16):
                count_copy(o, (me, y, c)).wait_recv()
                total = total + cnt_r_buf[o]
            pair_s_buf[...] = total
            pair.start()
            sent_all()
            for o in range(1, 16):
                count_copy(o, (me, y, c)).wait_send()
            summed(1)
            for h in range(2):
                for k in range(1, SIDE):
                    rs1_copy(k, h).wait_send()
                    ag_copy(k, (y - k + SIDE) % SIDE, h).wait_recv()
            for h in range(2):
                for k in range(1, SIDE):
                    ag_copy(k, y, h).wait_send()

        @pl.when(level == 1)
        def _():
            sent_all()
            for k in range(1, SIDE):
                rs2_copy(k, y).wait_recv()
            others = rs2_recv[0].astype(F32) + rs2_recv[1].astype(F32) + rs2_recv[2].astype(F32)
            for q in range(SIDE):

                @pl.when(y == q)
                def _():
                    own = slice(q * share_width, (q + 1) * share_width)
                    out_ref[...] = (x_buf[:, own].astype(F32) + (acc[:, own] + others)).T.astype(BF)

            for k in range(1, SIDE):
                rs2_copy(k, (y + k) % SIDE).wait_send()

        return 0

    lax.fori_loop(0, 2, layer, 0)
    pair.wait_recv()
    load_ref[...] = (pair_s_buf[...] + pair_r_buf[...])[0:1, 0:2]
    pair.wait_send()


def body(
    tokens, route_one, route_two, share_one, share_two, gain_one, gain_two, gate_up_one, down_one, gate_up_two, down_two
):
    count, width = tokens.shape
    ex = lax.axis_size("ex")
    top = route_one.shape[1]
    share_width = down_one.shape[1]
    cap = 2 * count * top // ex
    total = ex * cap
    vmem = pl.BlockSpec(memory_space=pltpu.VMEM)
    hbm = pl.BlockSpec(memory_space=pl.ANY)
    dma = pltpu.SemaphoreType.DMA

    def flat(gate_up):
        return jnp.transpose(gate_up[0], (1, 2, 0)).reshape(2 * share_width, width)

    mixed, load = pl.pallas_call(
        functools.partial(moe_kernel, cap),
        name="two_layers",
        out_shape=[jax.ShapeDtypeStruct((share_width, count), BF), jax.ShapeDtypeStruct((1, 2), I32)],
        in_specs=[vmem] * 7 + [hbm] * 4,
        out_specs=[vmem] * 2,
        scratch_shapes=[
            pltpu.VMEM((2 * share_width, width), BF),
            pltpu.VMEM((share_width, width), BF),
            pltpu.VMEM((count, width), BF),
            pltpu.VMEM((count, width), BF),
            pltpu.VMEM((2, ex, count), F32),
            pltpu.VMEM((2, ex, count), F32),
            pltpu.VMEM((2, ex, count), F32),
            pltpu.VMEM((total, width), BF),
            pltpu.VMEM((total, width), BF),
            pltpu.VMEM((total, width), BF),
            pltpu.VMEM((total * 3 // 4, width), BF),
            pltpu.VMEM((total // 2, width), BF),
            pltpu.VMEM((total, width), BF),
            pltpu.VMEM((count, width), F32),
            pltpu.VMEM((count, width), BF),
            pltpu.VMEM((SIDE - 1, count // SIDE, width), BF),
            pltpu.VMEM((SIDE, count, share_width), BF),
            pltpu.VMEM((SIDE - 1, count, share_width), BF),
            pltpu.VMEM((16, 8, 128), I32),
            pltpu.VMEM((16, 8, 128), I32),
            pltpu.VMEM((8, 128), I32),
            pltpu.VMEM((8, 128), I32),
            pltpu.VMEM((2, 1, width), F32),
            dma((2,)),
            dma((16,)), dma((16,)),
            dma((16, 3)), dma((16, 3)),
            dma((16, 3, 2)), dma((16, 3, 2)),
            dma((16, 2)), dma((16, 2)),
            dma((3, 3)), dma((3, 3)),
            dma((2, 3)), dma((2, 3)),
            dma((16,)), dma((16,)),
        ],
        compiler_params=pltpu.CompilerParams(
            collective_id=0, has_side_effects=True, vmem_limit_bytes=64 * 1024 * 1024 - 65536
        ),
    )(
        tokens.T, route_one.T, route_two.T, share_one.T, share_two.T, gain_one, gain_two,
        flat(gate_up_one), down_one[0], flat(gate_up_two), down_two[0],
    )
    return mixed.T, load.T


def solution(mesh):
    in_specs = (
        P(("ex", "dp"), None),
        P(("ex", "dp"), None),
        P(("ex", "dp"), None),
        P(("ex", "dp"), None),
        P(("ex", "dp"), None),
        P(),
        P(),
        P("ex", None, None, "tp"),
        P("ex", "tp", None),
        P("ex", None, None, "tp"),
        P("ex", "tp", None),
    )
    out_specs = (P(("ex", "dp"), "tp"), P(None, "ex"))
    return jax.shard_map(body, mesh=mesh, in_specs=in_specs, out_specs=out_specs, check_vma=False)
```
